32 devices in a mesh: win: 4 (over z), step: 8 (over y, x, core).
Axes of the slice: x: 2, y: 2, z: 4, core: 2. Of those that a mesh axis runs over, the one named last changes fastest.
Arguments:
- initial_state: float32 [32, 32, 128], replicated, may hold values from -6 to 6
- source: float32 [4, 8, 32, 32, 128], P('win', 'step'), may hold values from -6 to 6
- absorption: float32 [32, 32, 128], replicated, may hold values from 0.01 to 0.2
Outputs:
- state: float32 [4, 8, 32, 32, 128], P('win', 'step')
The draws below stay inside these ranges and needn't reach their ends.
All inputs are finite; a program needn't handle non-finite values.
Results may differ from the reference program's by a relative error of at most 0.00026.
Values sent between devices are 32-bit elements; how exact they have to be, the bound alone decides.
A program may use at most 64 MiB of HBM per device.

```python
import math
import jax
import jax.numpy as jnp

NX = 32
NY = 32
NZ = 128
ITERS = 2
SWEEPS = 8
STEPS = 8
WINDOWS = 4


def block_scale(rng, dims, split, low, largest):
    def one(dim, blocks):
        heights = jax.random.uniform(jax.random.fold_in(jax.random.fold_in(rng, 6), dim), (blocks,), jnp.float32, low / len(split), largest / len(split))
        return jnp.repeat(jnp.exp(heights), dims[dim] // blocks).reshape((-1,) + (1,) * (len(dims) - dim - 1))

    loudness = one(*split[0])
    for cut in split[1:]:
        loudness = loudness * one(*cut)
    return loudness


def centred(own_key, extent, spread, most, shards=(), kind=jnp.bfloat16):
    factor_of = block_scale(own_key, extent, shards, -0.22, 0.18) if shards else 1.0
    values = jax.random.normal(own_key, extent, jnp.float32) * spread * factor_of
    return jnp.minimum(jnp.maximum(values, -most), most).astype(kind)


def setup_inputs(seed: int = 0) -> dict:
    keys = jax.random.split(jax.random.key(seed), 4)
    initial_state = centred(keys[0], (NX, NY, NZ), 1.0, 6.0, (), jnp.float32)
    source = centred(keys[1], (WINDOWS, STEPS, NX, NY, NZ), 1.0, 6.0, ((0, 4), (1, 8)), jnp.float32)
    absorption = jnp.clip(jnp.exp(jax.random.uniform(keys[2], (NX, NY, NZ), jnp.float32, math.log(0.01), math.log(0.2))), 0.01, 0.2)
    return dict(initial_state=initial_state, source=source, absorption=absorption)


alpha_corner = 0.1
coupling = 0.05


def pad_cube(field):
    widths = [(0, 0)] * (field.ndim - 3) + [(1, 1)] * 3
    return jnp.pad(field, widths)


def neighbours(field):
    padded = pad_cube(field)
    total = padded[..., 2:, 1:-1, 1:-1] + padded[..., :-2, 1:-1, 1:-1]
    total = total + padded[..., 1:-1, 2:, 1:-1] + padded[..., 1:-1, :-2, 1:-1]
    total = total + padded[..., 1:-1, 1:-1, 2:] + padded[..., 1:-1, 1:-1, :-2]
    return total


def complex_times(first, second):
    return jnp.stack([first[0] * second[0] - first[1] * second[1], first[0] * second[1] + first[1] * second[0]])


def relax(spectrum, inverse):
    field = complex_times(inverse, spectrum)
    for repeat in range(SWEEPS - 1):
        field = complex_times(inverse, spectrum + coupling * neighbours(field))
    return field


def inverse_diagonal(angle, absorption, gamma):
    real_part = 1.0 - gamma * jnp.cos(angle) + absorption + 6.0 * coupling
    imag_part = jnp.broadcast_to(gamma * jnp.sin(angle), real_part.shape)
    magnitude = real_part * real_part + imag_part * imag_part
    return jnp.stack([real_part / magnitude, -imag_part / magnitude])


def reference(initial_state, source, absorption):
    gamma = alpha_corner ** (1.0 / STEPS)
    moments = jnp.arange(STEPS, dtype=jnp.float32)
    scale = (gamma ** moments)[None, :, None, None, None]
    angle = (moments * (2.0 * math.pi / STEPS))[:, None, None, None]
    inverse = inverse_diagonal(angle, absorption, gamma)[:, None]
    state = jnp.zeros_like(source)
    for repeat in range(ITERS):
        ends = state[:, -1]
        before = jnp.concatenate([initial_state[None], ends[:-1]], axis=0)
        forcing = source.at[:, 0].add(before - alpha_corner * ends)
        spectrum_full = jnp.fft.fft(forcing * scale, axis=1)
        field = relax(jnp.stack([spectrum_full.real, spectrum_full.imag]), inverse)
        state = jnp.fft.ifft(field[0] + 1j * field[1], axis=1).real / scale
    return state
```

```python
import functools
import math

import jax
import jax.numpy as jnp
from jax import lax
from jax.experimental import pallas as pl
from jax.experimental.pallas import tpu as pltpu
from jax.sharding import PartitionSpec as P

ITERS = 2
SWEEPS = 8


alpha_corner = 0.1
coupling = 0.05


def from_behind(block, axis, distance):
    devices = range(lax.axis_size(axis))
    route = [(i - distance, i) for i in devices if i - distance in devices]
    return lax.ppermute(block, axis, route)


def pad_cube(field):
    widths = [(0, 0)] * (field.ndim - 3) + [(1, 1)] * 3
    return jnp.pad(field, widths)


def neighbours(field):
    padded = pad_cube(field)
    total = padded[..., 2:, 1:-1, 1:-1] + padded[..., :-2, 1:-1, 1:-1]
    total = total + padded[..., 1:-1, 2:, 1:-1] + padded[..., 1:-1, :-2, 1:-1]
    total = total + padded[..., 1:-1, 1:-1, 2:] + padded[..., 1:-1, 1:-1, :-2]
    return total


def complex_times(first, second):
    return jnp.stack(
        [first[0] * second[0] - first[1] * second[1], first[0] * second[1] + first[1] * second[0]]
    )


def relax(spectrum, inverse):
    field = complex_times(inverse, spectrum)
    for repeat in range(SWEEPS - 1):
        field = complex_times(inverse, spectrum + coupling * neighbours(field))
    return field


def inverse_diagonal(angle, absorption, gamma):
    real_part = 1.0 - gamma * jnp.cos(angle) + absorption + 6.0 * coupling
    imag_part = jnp.broadcast_to(gamma * jnp.sin(angle), real_part.shape)
    magnitude = real_part * real_part + imag_part * imag_part
    return jnp.stack([real_part / magnitude, -imag_part / magnitude])


def dft_tables(window_len):
    index = jnp.arange(window_len, dtype=jnp.int32)
    product = index[:, None] * index[None, :] % window_len
    angle = product.astype(jnp.float32) * (2.0 * math.pi / window_len)
    return (jnp.cos(angle), jnp.sin(angle))


def transform_exchange(scaled, window_len):
    pencil = lax.all_to_all(scaled[None], "step", split_axis=1, concat_axis=0, tiled=True)
    cosine, sine = dft_tables(window_len)
    flat = pencil.reshape(window_len, -1)
    real_part = jnp.dot(cosine, flat, precision=lax.Precision.HIGHEST)
    imag_part = -jnp.dot(sine, flat, precision=lax.Precision.HIGHEST)
    shaped = pencil.shape
    spectrum = (
        lax.all_to_all(real_part.reshape(shaped), "step", split_axis=0, concat_axis=1, tiled=True),
        lax.all_to_all(imag_part.reshape(shaped), "step", split_axis=0, concat_axis=1, tiled=True),
    )
    return jnp.stack([spectrum[0][0], spectrum[1][0]])


def untransform_exchange(field, window_len):
    pencil = (
        lax.all_to_all(field[0][None], "step", split_axis=1, concat_axis=0, tiled=True),
        lax.all_to_all(field[1][None], "step", split_axis=1, concat_axis=0, tiled=True),
    )
    cosine, sine = dft_tables(window_len)
    shaped = pencil[0].shape
    values = jnp.dot(cosine, pencil[0].reshape(window_len, -1), precision=lax.Precision.HIGHEST)
    values = values - jnp.dot(
        sine, pencil[1].reshape(window_len, -1), precision=lax.Precision.HIGHEST
    )
    values = values / window_len
    result = lax.all_to_all(values.reshape(shaped), "step", split_axis=0, concat_axis=1, tiled=True)
    return result[0]


def per_device(initial_state, source, absorption):
    window_len = lax.axis_size("step")
    moment = lax.axis_index("step")
    window_index = lax.axis_index("win")
    gamma = alpha_corner ** (1.0 / window_len)
    scale = gamma ** moment.astype(jnp.float32)
    forcing_base = source[0, 0]
    is_first = moment == 0
    state = jnp.zeros_like(forcing_base)
    angle = moment.astype(jnp.float32) * (2.0 * math.pi / window_len)
    inverse = inverse_diagonal(angle, absorption, gamma)
    for repeat in range(ITERS):
        if repeat == 0:
            correction = jnp.where(window_index == 0, initial_state, 0.0)
        else:
            ends = from_behind(state, "step", 1 - window_len)
            before = from_behind(ends, "win", 1)
            before = jnp.where(window_index == 0, initial_state, before)
            correction = before - alpha_corner * ends
        forcing = forcing_base + jnp.where(is_first, correction, 0.0)
        scaled = forcing * scale
        spectrum = transform_exchange(scaled, window_len)
        field = relax(spectrum, inverse)
        values = untransform_exchange(field, window_len)
        state = values / scale
    return state[None, None]


LANES = 128
TILE = 8


def tables(length):
    gamma = alpha_corner ** (1.0 / length)
    into, back, angles = [], [], []
    for core in range(2):
        rows_in, rows_back = [], []
        for time in range(length):
            scale = gamma**time
            row_in, row_back = [], []
            for p in range(length // 4):
                j = 2 * p + core
                if j == 0:
                    pair, weight = (1.0, (-1.0) ** time), 1.0 / length
                else:
                    turn = 2.0 * math.pi * (j * time % length) / length
                    pair, weight = (math.cos(turn), -math.sin(turn)), 2.0 / length
                row_in += [value * scale / coupling for value in pair]
                row_back += [value * weight / scale for value in pair]
            rows_in.append(row_in)
            rows_back.append(row_back)
        into.append(rows_in)
        back.append(rows_back)
        angles.append([2.0 * math.pi * (2 * p + core) / length for p in range(length // 4)])
    return into, back, angles


def kernel(
    length, windows, nx, ny, ext, ey,
    source, initial, absorb, out,
    raw, first, absv, coef, base, fa, fb, corr,
    psend, pgot, ends, zgot, csend, qsend, qgot, obuf,
    lsem, asend, brecv, fsend, esem, zsem, csem_s, csem_r, qsem_s, qsem_r, osem_s, osem_r,
):
    half = length // 2
    gx, gy = half // 2, 2
    bs, bsy = nx // gx, ny // gy
    reach = SWEEPS - 1
    pairs = length // 4
    units = 2 * pairs
    gamma = alpha_corner ** (1.0 / length)
    into, back, angles = tables(length)
    me = lax.axis_index("step")
    w = lax.axis_index("win")
    core, m = me % 2, me // 2
    partner = m * 2 + (1 - core)
    bx, by = m % gx, m // gx

    def xlo(b):
        if gx == 2:
            return b * (nx - ext)
        return jnp.minimum(jnp.maximum(b * bs - reach, 0), nx - ext)

    def ylo(b):
        return pl.multiple_of(b * (ny - ey), TILE)

    def pick(a, b):
        return jnp.where(core == 0, jnp.float32(a), jnp.float32(b))

    def region(ref, b_x, b_y):
        return ref.at[pl.ds(xlo(b_x), ext), pl.ds(ylo(b_y), ey), :]

    ox = bx * bs - xlo(bx)
    oy = pl.multiple_of(by * bsy - ylo(by), TILE)

    loads = [
        pltpu.make_async_copy(region(absorb, bx, by), absv, lsem.at[0]),
        pltpu.make_async_copy(region(source, bx, by), raw.at[me], lsem.at[1]),
        pltpu.make_async_copy(region(initial, bx, by), first, lsem.at[2]),
    ]
    for load in loads:
        load.start()
    zero_row = jnp.zeros((ey, LANES), jnp.float32)
    for u in range(units):
        for ref in (fa, fb):
            ref[u, 0] = zero_row
            ref[u, ext + 1] = zero_row
    if gx > 2:
        corr[...] = jnp.zeros_like(corr)

    barrier = pltpu.get_barrier_semaphore()
    for d in range(1, length):
        pl.semaphore_signal(
            barrier, inc=1, device_id={"step": (me + d) % length}, device_id_type=pl.DeviceIdType.MESH
        )

    @pl.when(w > 0)
    def _():
        pl.semaphore_signal(barrier, inc=1, device_id={"win": w - 1}, device_id_type=pl.DeviceIdType.MESH)

    @pl.when(w < windows - 1)
    def _():
        pl.semaphore_signal(barrier, inc=1, device_id={"win": w + 1}, device_id_type=pl.DeviceIdType.MESH)

    nearby = jnp.where(w > 0, 1, 0) + jnp.where(w < windows - 1, 1, 0)
    pl.semaphore_wait(barrier, length - 1 + nearby)

    def remote(src, dst, send, recv, **where):
        return pltpu.make_async_remote_copy(
            src_ref=src, dst_ref=dst, send_sem=send, recv_sem=recv,
            device_id=where, device_id_type=pl.DeviceIdType.MESH,
        )

    outgoing = []
    for d in range(1, half):
        to = (m + d) % half
        copy = remote(
            region(source, to % gx, to // gx), raw.at[me], asend.at[d], brecv.at[me], step=to * 2 + core
        )
        copy.start()
        outgoing.append(copy)
    copy = remote(region(source, bx, by), raw.at[me], asend.at[0], brecv.at[me], step=partner)
    copy.start()
    outgoing.append(copy)

    loads[0].wait()

    def coefficients(i, carry):
        for p in range(pairs):
            rows = absv[i]
            cosine = pick(math.cos(angles[0][p]), math.cos(angles[1][p]))
            imag = pick(gamma * math.sin(angles[0][p]), gamma * math.sin(angles[1][p]))
            real = 1.0 - gamma * cosine + rows + 6.0 * coupling
            over = coupling / (real * real + imag * imag)
            coef[3 * p, i] = real * over
            coef[3 * p + 1, i] = -imag * over
            if p == 0:
                other = pick(-1.0, math.cos(angles[1][p]))
                real = 1.0 - gamma * other + rows + 6.0 * coupling
                over = coupling / (real * real + imag * imag)
                coef[3 * p + 2, i] = real * over
        return carry

    lax.fori_loop(0, ext, coefficients, 0)

    def weights(p, i):
        straight = coef[3 * p, i]
        return straight, (coef[3 * p + 2, i] if p == 0 else straight), coef[3 * p + 1, i]

    def arrival(t):
        return remote(raw.at[t], raw.at[t], asend.at[0], brecv.at[t], step=partner)

    for d in range(1, half):
        t = ((m + half - d) % half) * 2 + core
        arrival(t).wait_recv()
        copy = remote(raw.at[t], raw.at[t], fsend.at[d], brecv.at[t], step=partner)
        copy.start()
        outgoing.append(copy)
    for d in range(half):
        arrival(((m + half - d) % half) * 2 + (1 - core)).wait_recv()
    loads[1].wait()
    loads[2].wait()
    is_first = jnp.where(w == 0, jnp.float32(1.0 / coupling), jnp.float32(0.0))

    def second_weight(p, weight):
        return weight[2] + (pick(1.0, 0.0) * weight[1] if p == 0 else 0.0)

    def transform(i, carry):
        begin = first[i] * is_first
        fields = [raw[t, i] for t in range(length)]
        for p in range(pairs):
            weight = weights(p, i)
            s0, s1 = begin, begin * pick(1.0, 0.0) if p == 0 else None
            for t in range(length):
                s0 = s0 + pick(into[0][t][2 * p], into[1][t][2 * p]) * fields[t]
                term = pick(into[0][t][2 * p + 1], into[1][t][2 * p + 1]) * fields[t]
                s1 = term if s1 is None else s1 + term
            b0 = weight[0] * s0 - weight[2] * s1
            b1 = weight[1] * s1 + weight[2] * s0
            base[2 * p, i] = b0
            base[2 * p + 1, i] = b1
            fa[2 * p, i + 1] = b0
            fa[2 * p + 1, i + 1] = b1
        return carry

    lax.fori_loop(0, ext, transform, 0)

    lane = lax.broadcasted_iota(jnp.int32, (ey, LANES), 1)
    row = lax.broadcasted_iota(jnp.int32, (ey, LANES), 0)

    def around(ref, u, r):
        v = ref[u, r]
        total = ref[u, r - 1] + ref[u, r + 1]
        total = total + jnp.where(lane == 0, 0.0, pltpu.roll(v, 1, 1))
        total = total + jnp.where(lane == LANES - 1, 0.0, pltpu.roll(v, LANES - 1, 1))
        total = total + jnp.where(row == 0, 0.0, pltpu.roll(v, 1, 0))
        total = total + jnp.where(row == ey - 1, 0.0, pltpu.roll(v, ey - 1, 0))
        return total

    def sweeps():
        here, there = fa, fb
        for k in range(1, SWEEPS):
            begin, count = (bx * k, ext - k) if gx == 2 else (0, ext)

            def body(n, carry, here=here, there=there, begin=begin):
                i = begin + n
                for p in range(pairs):
                    weight = weights(p, i)
                    n0 = around(here, 2 * p, i + 1)
                    n1 = around(here, 2 * p + 1, i + 1)
                    there[2 * p, i + 1] = base[2 * p, i] + (weight[0] * n0 - weight[2] * n1)
                    there[2 * p + 1, i + 1] = base[2 * p + 1, i] + (weight[1] * n1 + weight[2] * n0)
                return carry

            lax.fori_loop(0, count, body, 0)
            here, there = there, here
        return here

    final = sweeps()

    def part(t, y0, rows):
        total = None
        for u in range(units):
            factor = pick(back[0][t[0]][u], back[1][t[1]][u])
            term = factor * final[u, pl.ds(ox + 1, bs), pl.ds(y0, rows), :]
            total = term if total is None else total + term
        return total

    last = (length - 1, length - 1)
    psend[...] = part(last, pl.multiple_of(oy + TILE * (1 - core), TILE), TILE)
    swap = remote(psend, pgot, esem.at[0], esem.at[1], step=partner)
    swap.start()
    mine = part(last, pl.multiple_of(oy + TILE * core, TILE), TILE)
    swap.wait_recv()
    mine = mine + pgot[...]
    ends[...] = mine
    outgoing.append(swap)

    onward = remote(ends, zgot, zsem.at[0], zsem.at[1], win=(w + 1) % windows)

    @pl.when(w < windows - 1)
    def _():
        onward.start()

    @pl.when(w == 0)
    def _():
        zgot[...] = jnp.zeros_like(zgot)

    @pl.when(w > 0)
    def _():
        onward.wait_recv()

    change = zgot[...] - alpha_corner * ends[...]
    csend[...] = change
    corr[pl.ds(ox, bs), pl.ds(pl.multiple_of(oy + TILE * core, TILE), TILE), :] = change

    def spread(ex, ey_, send):
        rows, skip = (bs, 0) if ex == 0 else (reach, bs - reach if ex == 1 else 0)
        tx, ty = (bx + ex, by + ey_) if send else (bx, by)
        fx, fy = (bx, by) if send else (bx - ex, by - ey_)
        ax, ay = (tx, ty) if send else (fx, fy)
        inside = (ax >= 0) & (ax < gx) & (ay >= 0) & (ay < gy)
        slot = ((ex + 1) * 3 + (ey_ + 1)) * 2
        for c in range(2):
            near = c == (1 if ey_ == 1 else 0)
            if send:
                okay = inside if ey_ == 0 else inside & (core == (1 if ey_ == 1 else 0))
                if ex == 0 and ey_ == 0:
                    okay = core != c
                fc, tc = core, c
            else:
                if ey_ != 0 and not near:
                    continue
                okay = inside
                if ex == 0 and ey_ == 0:
                    okay = core != c
                fc, tc = c, core

            @pl.when(okay)
            def _(c=c, fc=fc, tc=tc):
                copy = remote(
                    csend.at[pl.ds(skip, rows)],
                    corr.at[
                        pl.ds(fx * bs + skip - xlo(tx), rows),
                        pl.ds(pl.multiple_of(fy * bsy + TILE * fc - ylo(ty), TILE), TILE),
                        :,
                    ],
                    csem_s.at[slot + c],
                    csem_r.at[slot + fc],
                    step=(ty * gx + tx) * 2 + tc if send == 1 else partner,
                )
                if send == 1:
                    copy.start()
                elif send == 2:
                    copy.wait_send()
                else:
                    copy.wait_recv()

    offsets = [(ex, e) for ex in (-1, 0, 1) for e in (-1, 0, 1)]
    for ex, e in offsets:
        spread(ex, e, 1)
    for ex, e in offsets:
        spread(ex, e, 0)

    def correct(i, carry):
        x = corr[i] * (1.0 / coupling)
        for p in range(pairs):
            weight = weights(p, i)
            b0 = base[2 * p, i] + weight[0] * x
            b1 = base[2 * p + 1, i] + second_weight(p, weight) * x
            base[2 * p, i] = b0
            base[2 * p + 1, i] = b1
            fa[2 * p, i + 1] = b0
            fa[2 * p + 1, i + 1] = b1
        return carry

    lax.fori_loop(0, ext, correct, 0)
    final = sweeps()

    for k in range(half):
        qsend[k] = part((2 * k + 1, 2 * k), oy, bsy)
        copy = remote(qsend.at[k], qgot.at[k], qsem_s.at[k], qsem_r.at[k], step=partner)
        copy.start()
        outgoing.append(copy)
    for k in range(half):
        obuf[k] = part((2 * k, 2 * k + 1), oy, bsy)

    def place(b_x, b_y):
        return out.at[pl.ds(b_x * bs, bs), pl.ds(pl.multiple_of(b_y * bsy, TILE), bsy), :]

    for k in range(half):
        remote(qsend.at[k], qgot.at[k], qsem_s.at[k], qsem_r.at[k], step=partner).wait_recv()
        obuf[k] = obuf[k] + qgot[k]

        @pl.when(m == k)
        def _(k=k):
            pltpu.make_async_copy(obuf.at[k], place(bx, by), lsem.at[3]).start()

        @pl.when(m != k)
        def _(k=k):
            remote(obuf.at[k], place(bx, by), osem_s.at[k], osem_r.at[m], step=2 * k + core).start()

    for copy in outgoing:
        copy.wait_send()
    for ex, e in offsets:
        spread(ex, e, 2)

    @pl.when(w < windows - 1)
    def _():
        onward.wait_send()

    for k in range(half):

        @pl.when(m == k)
        def _(k=k):
            pltpu.make_async_copy(obuf.at[k], place(bx, by), lsem.at[3]).wait()

        @pl.when(m != k)
        def _(k=k):
            done = remote(obuf.at[k], place(k % gx, k // gx), osem_s.at[k], osem_r.at[k], step=partner)
            done.wait_send()
            done.wait_recv()


def blocks(initial_state, source, absorption):
    length = lax.axis_size("step")
    windows = lax.axis_size("win")
    nx, ny, nz = initial_state.shape
    half = length // 2
    gx, reach = half // 2, SWEEPS - 1
    bs, bsy = nx // gx, ny // 2
    ext = min(nx, bs + reach * (1 if gx == 2 else 2))
    ey = bsy + -(-reach // TILE) * TILE
    units = length // 2
    f32 = jnp.float32
    dma = pltpu.SemaphoreType.DMA
    return pl.pallas_call(
        functools.partial(kernel, length, windows, nx, ny, ext, ey),
        out_shape=jax.ShapeDtypeStruct((nx, ny, nz), f32),
        in_specs=[pl.BlockSpec(memory_space=pl.ANY)] * 3,
        out_specs=pl.BlockSpec(memory_space=pl.ANY),
        scratch_shapes=[
            pltpu.VMEM((length, ext, ey, nz), f32),
            pltpu.VMEM((ext, ey, nz), f32),
            pltpu.VMEM((ext, ey, nz), f32),
            pltpu.VMEM((3 * length // 4, ext, ey, nz), f32),
            pltpu.VMEM((units, ext, ey, nz), f32),
            pltpu.VMEM((units, ext + 2, ey, nz), f32),
            pltpu.VMEM((units, ext + 2, ey, nz), f32),
            pltpu.VMEM((ext, ey, nz), f32),
            pltpu.VMEM((bs, TILE, nz), f32),
            pltpu.VMEM((bs, TILE, nz), f32),
            pltpu.VMEM((bs, TILE, nz), f32),
            pltpu.VMEM((bs, TILE, nz), f32),
            pltpu.VMEM((bs, TILE, nz), f32),
            pltpu.VMEM((half, bs, bsy, nz), f32),
            pltpu.VMEM((half, bs, bsy, nz), f32),
            pltpu.VMEM((half, bs, bsy, nz), f32),
            dma((4,)),
            dma((half,)),
            dma((length,)),
            dma((half,)),
            dma((2,)),
            dma((2,)),
            dma((18,)),
            dma((18,)),
            dma((half,)),
            dma((half,)),
            dma((half,)),
            dma((half,)),
        ],
        compiler_params=pltpu.CompilerParams(
            collective_id=0, has_side_effects=True, vmem_limit_bytes=60 * 1024 * 1024
        ),
    )(source[0, 0], initial_state, absorption)[None, None]


def fits(mesh, shape):
    length = mesh.shape["step"]
    if length % 8 or shape[2] != LANES or shape[1] != 4 * TILE:
        return False
    gx = length // 4
    return shape[0] % gx == 0 and shape[0] // gx >= SWEEPS - 1


def solution(mesh):
    def body(initial_state, source, absorption):
        plan = blocks if fits(mesh, initial_state.shape) else per_device
        return plan(initial_state, source, absorption)

    return jax.shard_map(
        body,
        mesh=mesh,
        in_specs=(P(), P("win", "step", None, None, None), P()),
        out_specs=P("win", "step", None, None, None),
        check_vma=False,
    )
```

```python
import functools
import math

import jax
import jax.numpy as jnp
from jax import lax
from jax.experimental import pallas as pl
from jax.experimental.pallas import tpu as pltpu
from jax.sharding import PartitionSpec as P

ITERS = 2
SWEEPS = 8


alpha_corner = 0.1
coupling = 0.05


def from_behind(block, axis, distance):
    devices = range(lax.axis_size(axis))
    route = [(i - distance, i) for i in devices if i - distance in devices]
    return lax.ppermute(block, axis, route)


def pad_cube(field):
    widths = [(0, 0)] * (field.ndim - 3) + [(1, 1)] * 3
    return jnp.pad(field, widths)


def neighbours(field):
    padded = pad_cube(field)
    total = padded[..., 2:, 1:-1, 1:-1] + padded[..., :-2, 1:-1, 1:-1]
    total = total + padded[..., 1:-1, 2:, 1:-1] + padded[..., 1:-1, :-2, 1:-1]
    total = total + padded[..., 1:-1, 1:-1, 2:] + padded[..., 1:-1, 1:-1, :-2]
    return total


def complex_times(first, second):
    return jnp.stack(
        [first[0] * second[0] - first[1] * second[1], first[0] * second[1] + first[1] * second[0]]
    )


def relax(spectrum, inverse):
    field = complex_times(inverse, spectrum)
    for repeat in range(SWEEPS - 1):
        field = complex_times(inverse, spectrum + coupling * neighbours(field))
    return field


def inverse_diagonal(angle, absorption, gamma):
    real_part = 1.0 - gamma * jnp.cos(angle) + absorption + 6.0 * coupling
    imag_part = jnp.broadcast_to(gamma * jnp.sin(angle), real_part.shape)
    magnitude = real_part * real_part + imag_part * imag_part
    return jnp.stack([real_part / magnitude, -imag_part / magnitude])


def dft_tables(window_len):
    index = jnp.arange(window_len, dtype=jnp.int32)
    product = index[:, None] * index[None, :] % window_len
    angle = product.astype(jnp.float32) * (2.0 * math.pi / window_len)
    return (jnp.cos(angle), jnp.sin(angle))


def transform_exchange(scaled, window_len):
    pencil = lax.all_to_all(scaled[None], "step", split_axis=1, concat_axis=0, tiled=True)
    cosine, sine = dft_tables(window_len)
    flat = pencil.reshape(window_len, -1)
    real_part = jnp.dot(cosine, flat, precision=lax.Precision.HIGHEST)
    imag_part = -jnp.dot(sine, flat, precision=lax.Precision.HIGHEST)
    shaped = pencil.shape
    spectrum = (
        lax.all_to_all(real_part.reshape(shaped), "step", split_axis=0, concat_axis=1, tiled=True),
        lax.all_to_all(imag_part.reshape(shaped), "step", split_axis=0, concat_axis=1, tiled=True),
    )
    return jnp.stack([spectrum[0][0], spectrum[1][0]])


def untransform_exchange(field, window_len):
    pencil = (
        lax.all_to_all(field[0][None], "step", split_axis=1, concat_axis=0, tiled=True),
        lax.all_to_all(field[1][None], "step", split_axis=1, concat_axis=0, tiled=True),
    )
    cosine, sine = dft_tables(window_len)
    shaped = pencil[0].shape
    values = jnp.dot(cosine, pencil[0].reshape(window_len, -1), precision=lax.Precision.HIGHEST)
    values = values - jnp.dot(
        sine, pencil[1].reshape(window_len, -1), precision=lax.Precision.HIGHEST
    )
    values = values / window_len
    result = lax.all_to_all(values.reshape(shaped), "step", split_axis=0, concat_axis=1, tiled=True)
    return result[0]


def per_device(initial_state, source, absorption):
    window_len = lax.axis_size("step")
    moment = lax.axis_index("step")
    window_index = lax.axis_index("win")
    gamma = alpha_corner ** (1.0 / window_len)
    scale = gamma ** moment.astype(jnp.float32)
    forcing_base = source[0, 0]
    is_first = moment == 0
    state = jnp.zeros_like(forcing_base)
    angle = moment.astype(jnp.float32) * (2.0 * math.pi / window_len)
    inverse = inverse_diagonal(angle, absorption, gamma)
    for repeat in range(ITERS):
        if repeat == 0:
            correction = jnp.where(window_index == 0, initial_state, 0.0)
        else:
            ends = from_behind(state, "step", 1 - window_len)
            before = from_behind(ends, "win", 1)
            before = jnp.where(window_index == 0, initial_state, before)
            correction = before - alpha_corner * ends
        forcing = forcing_base + jnp.where(is_first, correction, 0.0)
        scaled = forcing * scale
        spectrum = transform_exchange(scaled, window_len)
        field = relax(spectrum, inverse)
        values = untransform_exchange(field, window_len)
        state = values / scale
    return state[None, None]


LANES = 128
TILE = 8
GROUP = 8


def tables(length):
    gamma = alpha_corner ** (1.0 / length)
    into, back, angles = [], [], []
    for core in range(2):
        rows_in, rows_back = [], []
        for time in range(length):
            scale = gamma**time
            row_in, row_back = [], []
            for p in range(length // 4):
                j = 2 * p + core
                if j == 0:
                    pair, weight = (1.0, (-1.0) ** time), 1.0 / length
                else:
                    turn = 2.0 * math.pi * (j * time % length) / length
                    pair, weight = (math.cos(turn), -math.sin(turn)), 2.0 / length
                row_in += [value * scale / coupling for value in pair]
                row_back += [value * weight / scale for value in pair]
            rows_in.append(row_in)
            rows_back.append(row_back)
        into.append(rows_in)
        back.append(rows_back)
        angles.append([2.0 * math.pi * (2 * p + core) / length for p in range(length // 4)])
    return into, back, angles


def kernel(
    length, windows, nx, ny, ext, ey,
    source, initial, absorb, out,
    raw, first, absv, coef, base, again, fa, fb, corr,
    psend, pgot, ends, zgot, csend, qsend, qgot, obuf,
    lsem, asend, brecv, fsend, esem, zsem, csem_s, csem_r, qsem_s, qsem_r, osem_s, osem_r,
):
    half = length // 2
    gx, gy = half // 2, 2
    bs, bsy = nx // gx, ny // gy
    reach = SWEEPS - 1
    pairs = length // 4
    units = 2 * pairs
    gamma = alpha_corner ** (1.0 / length)
    into, back, angles = tables(length)
    me = lax.axis_index("step")
    w = lax.axis_index("win")
    core, m = me % 2, me // 2
    partner = m * 2 + (1 - core)
    bx, by = m % gx, m // gx

    def xlo(b):
        if gx == 2:
            return b * (nx - ext)
        return jnp.minimum(jnp.maximum(b * bs - reach, 0), nx - ext)

    def ylo(b):
        return pl.multiple_of(b * (ny - ey), TILE)

    def pick(a, b):
        return jnp.where(core == 0, jnp.float32(a), jnp.float32(b))

    def region(ref, b_x, b_y):
        return ref.at[pl.ds(xlo(b_x), ext), pl.ds(ylo(b_y), ey), :]

    ox = bx * bs - xlo(bx)
    oy = pl.multiple_of(by * bsy - ylo(by), TILE)

    loads = [
        pltpu.make_async_copy(region(absorb, bx, by), absv, lsem.at[0]),
        pltpu.make_async_copy(region(source, bx, by), raw.at[me], lsem.at[1]),
        pltpu.make_async_copy(region(initial, bx, by), first, lsem.at[2]),
    ]
    for load in loads:
        load.start()
    zero_row = jnp.zeros((ey, LANES), jnp.float32)
    for u in range(units):
        for ref in (fa, fb):
            ref[u, 0, pl.ds(TILE, ey)] = zero_row
            ref[u, ext + 1, pl.ds(TILE, ey)] = zero_row
            for r in range(1, ext + 1):
                ref[u, r, pl.ds(0, TILE)] = zero_row[:TILE]
                ref[u, r, pl.ds(TILE + ey, TILE)] = zero_row[:TILE]
    if gx > 2:
        corr[...] = jnp.zeros_like(corr)

    barrier = pltpu.get_barrier_semaphore()
    for d in range(1, length):
        pl.semaphore_signal(
            barrier, inc=1, device_id={"step": (me + d) % length}, device_id_type=pl.DeviceIdType.MESH
        )

    @pl.when(w > 0)
    def _():
        pl.semaphore_signal(barrier, inc=1, device_id={"win": w - 1}, device_id_type=pl.DeviceIdType.MESH)

    @pl.when(w < windows - 1)
    def _():
        pl.semaphore_signal(barrier, inc=1, device_id={"win": w + 1}, device_id_type=pl.DeviceIdType.MESH)

    nearby = jnp.where(w > 0, 1, 0) + jnp.where(w < windows - 1, 1, 0)
    pl.semaphore_wait(barrier, length - 1 + nearby)

    def remote(src, dst, send, recv, **where):
        return pltpu.make_async_remote_copy(
            src_ref=src, dst_ref=dst, send_sem=send, recv_sem=recv,
            device_id=where, device_id_type=pl.DeviceIdType.MESH,
        )

    outgoing = []
    for d in range(1, half):
        to = (m + d) % half
        copy = remote(
            region(source, to % gx, to // gx), raw.at[me], asend.at[d], brecv.at[me], step=to * 2 + core
        )
        copy.start()
        outgoing.append(copy)
    copy = remote(region(source, bx, by), raw.at[me], asend.at[0], brecv.at[me], step=partner)
    copy.start()
    outgoing.append(copy)

    def grouped(begin, count, work, most=GROUP):
        size = min(most, count)

        def body(g, carry):
            work(begin + g * size, size)
            return carry

        lax.fori_loop(0, count // size, body, 0)
        if count % size:
            work(begin + count - size, size)

    def each(one):
        def work(start, rows):
            for n in range(rows):
                one(start + n)

        return work

    loads[0].wait()

    def coefficients(i):
        for p in range(pairs):
            rows = absv[i]
            cosine = pick(math.cos(angles[0][p]), math.cos(angles[1][p]))
            imag = pick(gamma * math.sin(angles[0][p]), gamma * math.sin(angles[1][p]))
            real = 1.0 - gamma * cosine + rows + 6.0 * coupling
            over = coupling / (real * real + imag * imag)
            coef[3 * p, i] = real * over
            coef[3 * p + 1, i] = -imag * over
            if p == 0:
                other = pick(-1.0, math.cos(angles[1][p]))
                real = 1.0 - gamma * other + rows + 6.0 * coupling
                over = coupling / (real * real + imag * imag)
                coef[3 * p + 2, i] = real * over

    grouped(0, ext, each(coefficients))

    def weights(p, i):
        straight = coef[3 * p, i]
        return straight, (coef[3 * p + 2, i] if p == 0 else straight), coef[3 * p + 1, i]

    def arrival(t):
        return remote(raw.at[t], raw.at[t], asend.at[0], brecv.at[t], step=partner)

    for d in range(1, half):
        t = ((m + half - d) % half) * 2 + core
        arrival(t).wait_recv()
        copy = remote(raw.at[t], raw.at[t], fsend.at[d], brecv.at[t], step=partner)
        copy.start()
        outgoing.append(copy)
    for d in range(half):
        arrival(((m + half - d) % half) * 2 + (1 - core)).wait_recv()
    loads[1].wait()
    loads[2].wait()
    is_first = jnp.where(w == 0, jnp.float32(1.0 / coupling), jnp.float32(0.0))

    def second_weight(p, weight):
        return weight[2] + (pick(1.0, 0.0) * weight[1] if p == 0 else 0.0)

    def transform(i):
        begin = first[i] * is_first
        fields = [raw[t, i] for t in range(length)]
        for p in range(pairs):
            weight = weights(p, i)
            s0, s1 = begin, begin * pick(1.0, 0.0) if p == 0 else None
            for t in range(length):
                s0 = s0 + pick(into[0][t][2 * p], into[1][t][2 * p]) * fields[t]
                term = pick(into[0][t][2 * p + 1], into[1][t][2 * p + 1]) * fields[t]
                s1 = term if s1 is None else s1 + term
            b0 = weight[0] * s0 - weight[2] * s1
            b1 = weight[1] * s1 + weight[2] * s0
            base[2 * p, i] = b0
            base[2 * p + 1, i] = b1
            fa[2 * p, i + 1, pl.ds(TILE, ey)] = b0
            fa[2 * p + 1, i + 1, pl.ds(TILE, ey)] = b1

    grouped(0, ext, each(transform), GROUP // 2)

    lane = lax.broadcasted_iota(jnp.int32, (ey, LANES), 1)

    def around(ref, u, r):
        v = ref[u, r, pl.ds(TILE, ey)]
        total = jnp.where(lane == 0, 0.0, pltpu.roll(v, 1, 1))
        total = total + jnp.where(lane == LANES - 1, 0.0, pltpu.roll(v, LANES - 1, 1))
        beside = ref[u, r - 1, pl.ds(TILE, ey)] + ref[u, r + 1, pl.ds(TILE, ey)]
        return total + (beside + (ref[u, r, pl.ds(TILE - 1, ey)] + ref[u, r, pl.ds(TILE + 1, ey)]))

    def sweep_rows(base, here, there, start, rows):
        for n in range(rows):
            i = start + n
            for p in range(pairs):
                weight = weights(p, i)
                n0 = around(here, 2 * p, i + 1)
                n1 = around(here, 2 * p + 1, i + 1)
                there[2 * p, i + 1, pl.ds(TILE, ey)] = base[2 * p, i] + (weight[0] * n0 - weight[2] * n1)
                there[2 * p + 1, i + 1, pl.ds(TILE, ey)] = base[2 * p + 1, i] + (
                    weight[1] * n1 + weight[2] * n0
                )

    def sweeps(base):
        here, there = fa, fb
        for k in range(1, SWEEPS):
            begin, count = (bx * k, ext - k) if gx == 2 else (0, ext)
            grouped(begin, count, functools.partial(sweep_rows, base, here, there))
            here, there = there, here
        return here

    final = sweeps(base)

    def part(t, y0, rows):
        total = None
        for u in range(units):
            factor = pick(back[0][t[0]][u], back[1][t[1]][u])
            term = factor * final[u, pl.ds(ox + 1, bs), pl.ds(y0 + TILE, rows), :]
            total = term if total is None else total + term
        return total

    last = (length - 1, length - 1)
    psend[...] = part(last, pl.multiple_of(oy + TILE * (1 - core), TILE), TILE)
    swap = remote(psend, pgot, esem.at[0], esem.at[1], step=partner)
    swap.start()
    mine = part(last, pl.multiple_of(oy + TILE * core, TILE), TILE)
    swap.wait_recv()
    mine = mine + pgot[...]
    ends[...] = mine
    outgoing.append(swap)

    onward = remote(ends, zgot, zsem.at[0], zsem.at[1], win=(w + 1) % windows)

    @pl.when(w < windows - 1)
    def _():
        onward.start()

    @pl.when(w == 0)
    def _():
        zgot[...] = jnp.zeros_like(zgot)

    @pl.when(w > 0)
    def _():
        onward.wait_recv()

    change = zgot[...] - alpha_corner * ends[...]
    csend[...] = change
    corr[pl.ds(ox, bs), pl.ds(pl.multiple_of(oy + TILE * core, TILE), TILE), :] = change

    def spread(ex, ey_, send):
        rows, skip = (bs, 0) if ex == 0 else (reach, bs - reach if ex == 1 else 0)
        tx, ty = (bx + ex, by + ey_) if send else (bx, by)
        fx, fy = (bx, by) if send else (bx - ex, by - ey_)
        ax, ay = (tx, ty) if send else (fx, fy)
        inside = (ax >= 0) & (ax < gx) & (ay >= 0) & (ay < gy)
        slot = ((ex + 1) * 3 + (ey_ + 1)) * 2
        for c in range(2):
            near = c == (1 if ey_ == 1 else 0)
            if send:
                okay = inside if ey_ == 0 else inside & (core == (1 if ey_ == 1 else 0))
                if ex == 0 and ey_ == 0:
                    okay = core != c
                fc, tc = core, c
            else:
                if ey_ != 0 and not near:
                    continue
                okay = inside
                if ex == 0 and ey_ == 0:
                    okay = core != c
                fc, tc = c, core

            @pl.when(okay)
            def _(c=c, fc=fc, tc=tc):
                copy = remote(
                    csend.at[pl.ds(skip, rows)],
                    corr.at[
                        pl.ds(fx * bs + skip - xlo(tx), rows),
                        pl.ds(pl.multiple_of(fy * bsy + TILE * fc - ylo(ty), TILE), TILE),
                        :,
                    ],
                    csem_s.at[slot + c],
                    csem_r.at[slot + fc],
                    step=(ty * gx + tx) * 2 + tc if send == 1 else partner,
                )
                if send == 1:
                    copy.start()
                elif send == 2:
                    copy.wait_send()
                else:
                    copy.wait_recv()

    offsets = [(ex, e) for ex in (-1, 0, 1) for e in (-1, 0, 1)]
    for ex, e in offsets:
        spread(ex, e, 1)
    for ex, e in offsets:
        spread(ex, e, 0)

    def correct(i):
        x = corr[i] * (1.0 / coupling)
        for p in range(pairs):
            weight = weights(p, i)
            b0 = base[2 * p, i] + weight[0] * x
            b1 = base[2 * p + 1, i] + second_weight(p, weight) * x
            again[2 * p, i] = b0
            again[2 * p + 1, i] = b1
            fa[2 * p, i + 1, pl.ds(TILE, ey)] = b0
            fa[2 * p + 1, i + 1, pl.ds(TILE, ey)] = b1

    grouped(0, ext, each(correct))
    final = sweeps(again)

    for k in range(half):
        qsend[k] = part((2 * k + 1, 2 * k), oy, bsy)
        copy = remote(qsend.at[k], qgot.at[k], qsem_s.at[k], qsem_r.at[k], step=partner)
        copy.start()
        outgoing.append(copy)
    for k in range(half):
        obuf[k] = part((2 * k, 2 * k + 1), oy, bsy)

    def place(b_x, b_y):
        return out.at[pl.ds(b_x * bs, bs), pl.ds(pl.multiple_of(b_y * bsy, TILE), bsy), :]

    for k in range(half):
        remote(qsend.at[k], qgot.at[k], qsem_s.at[k], qsem_r.at[k], step=partner).wait_recv()
        obuf[k] = obuf[k] + qgot[k]

        @pl.when(m == k)
        def _(k=k):
            pltpu.make_async_copy(obuf.at[k], place(bx, by), lsem.at[3]).start()

        @pl.when(m != k)
        def _(k=k):
            remote(obuf.at[k], place(bx, by), osem_s.at[k], osem_r.at[m], step=2 * k + core).start()

    for copy in outgoing:
        copy.wait_send()
    for ex, e in offsets:
        spread(ex, e, 2)

    @pl.when(w < windows - 1)
    def _():
        onward.wait_send()

    for k in range(half):

        @pl.when(m == k)
        def _(k=k):
            pltpu.make_async_copy(obuf.at[k], place(bx, by), lsem.at[3]).wait()

        @pl.when(m != k)
        def _(k=k):
            done = remote(obuf.at[k], place(k % gx, k // gx), osem_s.at[k], osem_r.at[k], step=partner)
            done.wait_send()
            done.wait_recv()


def blocks(initial_state, source, absorption):
    length = lax.axis_size("step")
    windows = lax.axis_size("win")
    nx, ny, nz = initial_state.shape
    half = length // 2
    gx, reach = half // 2, SWEEPS - 1
    bs, bsy = nx // gx, ny // 2
    ext = min(nx, bs + reach * (1 if gx == 2 else 2))
    ey = bsy + -(-reach // TILE) * TILE
    units = length // 2
    f32 = jnp.float32
    dma = pltpu.SemaphoreType.DMA
    return pl.pallas_call(
        functools.partial(kernel, length, windows, nx, ny, ext, ey),
        out_shape=jax.ShapeDtypeStruct((nx, ny, nz), f32),
        in_specs=[pl.BlockSpec(memory_space=pl.ANY)] * 3,
        out_specs=pl.BlockSpec(memory_space=pl.ANY),
        scratch_shapes=[
            pltpu.VMEM((length, ext, ey, nz), f32),
            pltpu.VMEM((ext, ey, nz), f32),
            pltpu.VMEM((ext, ey, nz), f32),
            pltpu.VMEM((3 * length // 4, ext, ey, nz), f32),
            pltpu.VMEM((units, ext, ey, nz), f32),
            pltpu.VMEM((units, ext, ey, nz), f32),
            pltpu.VMEM((units, ext + 2, ey + 2 * TILE, nz), f32),
            pltpu.VMEM((units, ext + 2, ey + 2 * TILE, nz), f32),
            pltpu.VMEM((ext, ey, nz), f32),
            pltpu.VMEM((bs, TILE, nz), f32),
            pltpu.VMEM((bs, TILE, nz), f32),
            pltpu.VMEM((bs, TILE, nz), f32),
            pltpu.VMEM((bs, TILE, nz), f32),
            pltpu.VMEM((bs, TILE, nz), f32),
            pltpu.VMEM((half, bs, bsy, nz), f32),
            pltpu.VMEM((half, bs, bsy, nz), f32),
            pltpu.VMEM((half, bs, bsy, nz), f32),
            dma((4,)),
            dma((half,)),
            dma((length,)),
            dma((half,)),
            dma((2,)),
            dma((2,)),
            dma((18,)),
            dma((18,)),
            dma((half,)),
            dma((half,)),
            dma((half,)),
            dma((half,)),
        ],
        compiler_params=pltpu.CompilerParams(
            collective_id=0, has_side_effects=True, vmem_limit_bytes=28 * 1024 * 1024
        ),
    )(source[0, 0], initial_state, absorption)[None, None]


def fits(mesh, shape):
    length = mesh.shape["step"]
    if length % 8 or shape[2] != LANES or shape[1] != 4 * TILE:
        return False
    gx = length // 4
    return shape[0] % gx == 0 and shape[0] // gx >= SWEEPS - 1


def solution(mesh):
    def body(initial_state, source, absorption):
        plan = blocks if fits(mesh, initial_state.shape) else per_device
        return plan(initial_state, source, absorption)

    return jax.shard_map(
        body,
        mesh=mesh,
        in_specs=(P(), P("win", "step", None, None, None), P()),
        out_specs=P("win", "step", None, None, None),
        check_vma=False,
    )
```

```python
import functools
import math

import jax
import jax.numpy as jnp
from jax import lax
from jax.experimental import pallas as pl
from jax.experimental.pallas import tpu as pltpu
from jax.sharding import PartitionSpec as P

ITERS = 2
SWEEPS = 8


alpha_corner = 0.1
coupling = 0.05


def from_behind(block, axis, distance):
    devices = range(lax.axis_size(axis))
    route = [(i - distance, i) for i in devices if i - distance in devices]
    return lax.ppermute(block, axis, route)


def pad_cube(field):
    widths = [(0, 0)] * (field.ndim - 3) + [(1, 1)] * 3
    return jnp.pad(field, widths)


def neighbours(field):
    padded = pad_cube(field)
    total = padded[..., 2:, 1:-1, 1:-1] + padded[..., :-2, 1:-1, 1:-1]
    total = total + padded[..., 1:-1, 2:, 1:-1] + padded[..., 1:-1, :-2, 1:-1]
    total = total + padded[..., 1:-1, 1:-1, 2:] + padded[..., 1:-1, 1:-1, :-2]
    return total


def complex_times(first, second):
    return jnp.stack(
        [first[0] * second[0] - first[1] * second[1], first[0] * second[1] + first[1] * second[0]]
    )


def relax(spectrum, inverse):
    field = complex_times(inverse, spectrum)
    for repeat in range(SWEEPS - 1):
        field = complex_times(inverse, spectrum + coupling * neighbours(field))
    return field


def inverse_diagonal(angle, absorption, gamma):
    real_part = 1.0 - gamma * jnp.cos(angle) + absorption + 6.0 * coupling
    imag_part = jnp.broadcast_to(gamma * jnp.sin(angle), real_part.shape)
    magnitude = real_part * real_part + imag_part * imag_part
    return jnp.stack([real_part / magnitude, -imag_part / magnitude])


def dft_tables(window_len):
    index = jnp.arange(window_len, dtype=jnp.int32)
    product = index[:, None] * index[None, :] % window_len
    angle = product.astype(jnp.float32) * (2.0 * math.pi / window_len)
    return (jnp.cos(angle), jnp.sin(angle))


def transform_exchange(scaled, window_len):
    pencil = lax.all_to_all(scaled[None], "step", split_axis=1, concat_axis=0, tiled=True)
    cosine, sine = dft_tables(window_len)
    flat = pencil.reshape(window_len, -1)
    real_part = jnp.dot(cosine, flat, precision=lax.Precision.HIGHEST)
    imag_part = -jnp.dot(sine, flat, precision=lax.Precision.HIGHEST)
    shaped = pencil.shape
    spectrum = (
        lax.all_to_all(real_part.reshape(shaped), "step", split_axis=0, concat_axis=1, tiled=True),
        lax.all_to_all(imag_part.reshape(shaped), "step", split_axis=0, concat_axis=1, tiled=True),
    )
    return jnp.stack([spectrum[0][0], spectrum[1][0]])


def untransform_exchange(field, window_len):
    pencil = (
        lax.all_to_all(field[0][None], "step", split_axis=1, concat_axis=0, tiled=True),
        lax.all_to_all(field[1][None], "step", split_axis=1, concat_axis=0, tiled=True),
    )
    cosine, sine = dft_tables(window_len)
    shaped = pencil[0].shape
    values = jnp.dot(cosine, pencil[0].reshape(window_len, -1), precision=lax.Precision.HIGHEST)
    values = values - jnp.dot(
        sine, pencil[1].reshape(window_len, -1), precision=lax.Precision.HIGHEST
    )
    values = values / window_len
    result = lax.all_to_all(values.reshape(shaped), "step", split_axis=0, concat_axis=1, tiled=True)
    return result[0]


def per_device(initial_state, source, absorption):
    window_len = lax.axis_size("step")
    moment = lax.axis_index("step")
    window_index = lax.axis_index("win")
    gamma = alpha_corner ** (1.0 / window_len)
    scale = gamma ** moment.astype(jnp.float32)
    forcing_base = source[0, 0]
    is_first = moment == 0
    state = jnp.zeros_like(forcing_base)
    angle = moment.astype(jnp.float32) * (2.0 * math.pi / window_len)
    inverse = inverse_diagonal(angle, absorption, gamma)
    for repeat in range(ITERS):
        if repeat == 0:
            correction = jnp.where(window_index == 0, initial_state, 0.0)
        else:
            ends = from_behind(state, "step", 1 - window_len)
            before = from_behind(ends, "win", 1)
            before = jnp.where(window_index == 0, initial_state, before)
            correction = before - alpha_corner * ends
        forcing = forcing_base + jnp.where(is_first, correction, 0.0)
        scaled = forcing * scale
        spectrum = transform_exchange(scaled, window_len)
        field = relax(spectrum, inverse)
        values = untransform_exchange(field, window_len)
        state = values / scale
    return state[None, None]


LANES = 128
TILE = 8
GROUP = 8


def tables(length):
    gamma = alpha_corner ** (1.0 / length)
    into, back, angles = [], [], []
    for core in range(2):
        rows_in, rows_back = [], []
        for time in range(length):
            scale = gamma**time
            row_in, row_back = [], []
            for p in range(length // 4):
                j = 2 * p + core
                if j == 0:
                    pair, weight = (1.0, (-1.0) ** time), 1.0 / length
                else:
                    turn = 2.0 * math.pi * (j * time % length) / length
                    pair, weight = (math.cos(turn), -math.sin(turn)), 2.0 / length
                row_in += [value * scale / coupling for value in pair]
                row_back += [value * weight / scale for value in pair]
            rows_in.append(row_in)
            rows_back.append(row_back)
        into.append(rows_in)
        back.append(rows_back)
        angles.append([2.0 * math.pi * (2 * p + core) / length for p in range(length // 4)])
    return into, back, angles


def kernel(
    length, windows, nx, ny, ext, ey,
    source, initial, absorb, out,
    raw, first, absv, coef, base, again, fa, fb, corr,
    psend, pgot, ends, zgot, csend, qsend, qgot, obuf,
    lsem, asend, brecv, fsend, esem, zsem, csem_s, csem_r, qsem_s, qsem_r, osem_s, osem_r,
):
    half = length // 2
    gx, gy = half // 2, 2
    bs, bsy = nx // gx, ny // gy
    reach = SWEEPS - 1
    pairs = length // 4
    units = 2 * pairs
    gamma = alpha_corner ** (1.0 / length)
    into, back, angles = tables(length)
    me = lax.axis_index("step")
    w = lax.axis_index("win")
    core, m = me % 2, me // 2
    partner = m * 2 + (1 - core)
    bx, by = m % gx, m // gx

    def xlo(b):
        if gx == 2:
            return b * (nx - ext)
        return jnp.minimum(jnp.maximum(b * bs - reach, 0), nx - ext)

    def ylo(b):
        return pl.multiple_of(b * (ny - ey), TILE)

    def pick(a, b):
        return jnp.where(core == 0, jnp.float32(a), jnp.float32(b))

    def region(ref, b_x, b_y):
        return ref.at[pl.ds(xlo(b_x), ext), pl.ds(ylo(b_y), ey), :]

    ox = bx * bs - xlo(bx)
    oy = pl.multiple_of(by * bsy - ylo(by), TILE)

    loads = [
        pltpu.make_async_copy(region(absorb, bx, by), absv, lsem.at[0]),
        pltpu.make_async_copy(region(source, bx, by), raw.at[me], lsem.at[1]),
        pltpu.make_async_copy(region(initial, bx, by), first, lsem.at[2]),
    ]
    for load in loads:
        load.start()
    zero_row = jnp.zeros((ey, LANES), jnp.float32)
    for u in range(units):
        for ref in (fa, fb):
            ref[u, 0, pl.ds(TILE, ey)] = zero_row
            ref[u, ext + 1, pl.ds(TILE, ey)] = zero_row
            for r in range(1, ext + 1):
                ref[u, r, pl.ds(0, TILE)] = zero_row[:TILE]
                ref[u, r, pl.ds(TILE + ey, TILE)] = zero_row[:TILE]
    if gx > 2:
        corr[...] = jnp.zeros_like(corr)

    barrier = pltpu.get_barrier_semaphore()
    for d in range(1, length):
        pl.semaphore_signal(
            barrier, inc=1, device_id={"step": (me + d) % length}, device_id_type=pl.DeviceIdType.MESH
        )

    @pl.when(w > 0)
    def _():
        pl.semaphore_signal(barrier, inc=1, device_id={"win": w - 1}, device_id_type=pl.DeviceIdType.MESH)

    @pl.when(w < windows - 1)
    def _():
        pl.semaphore_signal(barrier, inc=1, device_id={"win": w + 1}, device_id_type=pl.DeviceIdType.MESH)

    nearby = jnp.where(w > 0, 1, 0) + jnp.where(w < windows - 1, 1, 0)
    pl.semaphore_wait(barrier, length - 1 + nearby)

    def remote(src, dst, send, recv, **where):
        return pltpu.make_async_remote_copy(
            src_ref=src, dst_ref=dst, send_sem=send, recv_sem=recv,
            device_id=where, device_id_type=pl.DeviceIdType.MESH,
        )

    outgoing = []
    for d in range(1, half):
        to = (m + d) % half
        copy = remote(
            region(source, to % gx, to // gx), raw.at[me], asend.at[d], brecv.at[me], step=to * 2 + core
        )
        copy.start()
        outgoing.append(copy)
    copy = remote(region(source, bx, by), raw.at[me], asend.at[0], brecv.at[me], step=partner)
    copy.start()
    outgoing.append(copy)

    def grouped(begin, count, work, most=GROUP):
        size = -(-count // max(1, count // most))

        def body(g, carry):
            work(begin + g * size, size)
            return carry

        lax.fori_loop(0, count // size, body, 0)
        if count % size:
            work(begin + count - size, size)

    def each(one):
        def work(start, rows):
            for n in range(rows):
                one(start + n)

        return work

    loads[0].wait()

    def coefficients(i):
        for p in range(pairs):
            rows = absv[i]
            cosine = pick(math.cos(angles[0][p]), math.cos(angles[1][p]))
            imag = pick(gamma * math.sin(angles[0][p]), gamma * math.sin(angles[1][p]))
            real = 1.0 - gamma * cosine + rows + 6.0 * coupling
            over = coupling / (real * real + imag * imag)
            coef[3 * p, i] = real * over
            coef[3 * p + 1, i] = -imag * over
            if p == 0:
                other = pick(-1.0, math.cos(angles[1][p]))
                real = 1.0 - gamma * other + rows + 6.0 * coupling
                over = coupling / (real * real + imag * imag)
                coef[3 * p + 2, i] = real * over

    grouped(0, ext, each(coefficients))

    def weights(p, i):
        straight = coef[3 * p, i]
        return straight, (coef[3 * p + 2, i] if p == 0 else straight), coef[3 * p + 1, i]

    def arrival(t):
        return remote(raw.at[t], raw.at[t], asend.at[0], brecv.at[t], step=partner)

    for d in range(1, half):
        t = ((m + half - d) % half) * 2 + core
        arrival(t).wait_recv()
        copy = remote(raw.at[t], raw.at[t], fsend.at[d], brecv.at[t], step=partner)
        copy.start()
        outgoing.append(copy)
    for d in range(half):
        arrival(((m + half - d) % half) * 2 + (1 - core)).wait_recv()
    loads[1].wait()
    loads[2].wait()
    is_first = jnp.where(w == 0, jnp.float32(1.0 / coupling), jnp.float32(0.0))

    def second_weight(p, weight):
        return weight[2] + (pick(1.0, 0.0) * weight[1] if p == 0 else 0.0)

    def transform(i):
        begin = first[i] * is_first
        fields = [raw[t, i] for t in range(length)]
        for p in range(pairs):
            weight = weights(p, i)
            s0, s1 = begin, begin * pick(1.0, 0.0) if p == 0 else None
            for t in range(length):
                s0 = s0 + pick(into[0][t][2 * p], into[1][t][2 * p]) * fields[t]
                term = pick(into[0][t][2 * p + 1], into[1][t][2 * p + 1]) * fields[t]
                s1 = term if s1 is None else s1 + term
            b0 = weight[0] * s0 - weight[2] * s1
            b1 = weight[1] * s1 + weight[2] * s0
            base[2 * p, i] = b0
            base[2 * p + 1, i] = b1
            fa[2 * p, i + 1, pl.ds(TILE, ey)] = b0
            fa[2 * p + 1, i + 1, pl.ds(TILE, ey)] = b1

    grouped(0, ext, each(transform), GROUP // 2)

    lane = lax.broadcasted_iota(jnp.int32, (ey, LANES), 1)

    def around(ref, u, r):
        v = ref[u, r, pl.ds(TILE, ey)]
        total = jnp.where(lane == 0, 0.0, pltpu.roll(v, 1, 1))
        total = total + jnp.where(lane == LANES - 1, 0.0, pltpu.roll(v, LANES - 1, 1))
        beside = ref[u, r - 1, pl.ds(TILE, ey)] + ref[u, r + 1, pl.ds(TILE, ey)]
        return total + (beside + (ref[u, r, pl.ds(TILE - 1, ey)] + ref[u, r, pl.ds(TILE + 1, ey)]))

    def sweep_rows(base, here, there, start, rows):
        for n in range(rows):
            i = start + n
            for p in range(pairs):
                weight = weights(p, i)
                n0 = around(here, 2 * p, i + 1)
                n1 = around(here, 2 * p + 1, i + 1)
                there[2 * p, i + 1, pl.ds(TILE, ey)] = base[2 * p, i] + (weight[0] * n0 - weight[2] * n1)
                there[2 * p + 1, i + 1, pl.ds(TILE, ey)] = base[2 * p + 1, i] + (
                    weight[1] * n1 + weight[2] * n0
                )

    def sweeps(base):
        here, there = fa, fb
        for k in range(1, SWEEPS):
            begin, count = (bx * k, ext - k) if gx == 2 else (0, ext)
            grouped(begin, count, functools.partial(sweep_rows, base, here, there))
            here, there = there, here
        return here

    final = sweeps(base)

    def part(t, y0, rows):
        total = None
        for u in range(units):
            factor = pick(back[0][t[0]][u], back[1][t[1]][u])
            term = factor * final[u, pl.ds(ox + 1, bs), pl.ds(y0 + TILE, rows), :]
            total = term if total is None else total + term
        return total

    last = (length - 1, length - 1)
    psend[...] = part(last, pl.multiple_of(oy + TILE * (1 - core), TILE), TILE)
    swap = remote(psend, pgot, esem.at[0], esem.at[1], step=partner)
    swap.start()
    mine = part(last, pl.multiple_of(oy + TILE * core, TILE), TILE)
    swap.wait_recv()
    mine = mine + pgot[...]
    ends[...] = mine
    outgoing.append(swap)

    onward = remote(ends, zgot, zsem.at[0], zsem.at[1], win=(w + 1) % windows)

    @pl.when(w < windows - 1)
    def _():
        onward.start()

    @pl.when(w == 0)
    def _():
        zgot[...] = jnp.zeros_like(zgot)

    @pl.when(w > 0)
    def _():
        onward.wait_recv()

    change = zgot[...] - alpha_corner * ends[...]
    csend[...] = change
    corr[pl.ds(ox, bs), pl.ds(pl.multiple_of(oy + TILE * core, TILE), TILE), :] = change

    def spread(ex, ey_, send):
        rows, skip = (bs, 0) if ex == 0 else (reach, bs - reach if ex == 1 else 0)
        tx, ty = (bx + ex, by + ey_) if send else (bx, by)
        fx, fy = (bx, by) if send else (bx - ex, by - ey_)
        ax, ay = (tx, ty) if send else (fx, fy)
        inside = (ax >= 0) & (ax < gx) & (ay >= 0) & (ay < gy)
        slot = ((ex + 1) * 3 + (ey_ + 1)) * 2
        for c in range(2):
            near = c == (1 if ey_ == 1 else 0)
            if send:
                okay = inside if ey_ == 0 else inside & (core == (1 if ey_ == 1 else 0))
                if ex == 0 and ey_ == 0:
                    okay = core != c
                fc, tc = core, c
            else:
                if ey_ != 0 and not near:
                    continue
                okay = inside
                if ex == 0 and ey_ == 0:
                    okay = core != c
                fc, tc = c, core

            @pl.when(okay)
            def _(c=c, fc=fc, tc=tc):
                copy = remote(
                    csend.at[pl.ds(skip, rows)],
                    corr.at[
                        pl.ds(fx * bs + skip - xlo(tx), rows),
                        pl.ds(pl.multiple_of(fy * bsy + TILE * fc - ylo(ty), TILE), TILE),
                        :,
                    ],
                    csem_s.at[slot + c],
                    csem_r.at[slot + fc],
                    step=(ty * gx + tx) * 2 + tc if send == 1 else partner,
                )
                if send == 1:
                    copy.start()
                elif send == 2:
                    copy.wait_send()
                else:
                    copy.wait_recv()

    offsets = [(ex, e) for ex in (-1, 0, 1) for e in (-1, 0, 1)]
    for ex, e in offsets:
        spread(ex, e, 1)
    for ex, e in offsets:
        spread(ex, e, 0)

    def correct(i):
        x = corr[i] * (1.0 / coupling)
        for p in range(pairs):
            weight = weights(p, i)
            b0 = base[2 * p, i] + weight[0] * x
            b1 = base[2 * p + 1, i] + second_weight(p, weight) * x
            again[2 * p, i] = b0
            again[2 * p + 1, i] = b1
            fa[2 * p, i + 1, pl.ds(TILE, ey)] = b0
            fa[2 * p + 1, i + 1, pl.ds(TILE, ey)] = b1

    grouped(0, ext, each(correct))
    final = sweeps(again)

    for k in range(half):
        qsend[k] = part((2 * k + 1, 2 * k), oy, bsy)
        copy = remote(qsend.at[k], qgot.at[k], qsem_s.at[k], qsem_r.at[k], step=partner)
        copy.start()
        outgoing.append(copy)
    for k in range(half):
        obuf[k] = part((2 * k, 2 * k + 1), oy, bsy)

    def place(b_x, b_y):
        return out.at[pl.ds(b_x * bs, bs), pl.ds(pl.multiple_of(b_y * bsy, TILE), bsy), :]

    for k in range(half):
        remote(qsend.at[k], qgot.at[k], qsem_s.at[k], qsem_r.at[k], step=partner).wait_recv()
        obuf[k] = obuf[k] + qgot[k]

        @pl.when(m == k)
        def _(k=k):
            pltpu.make_async_copy(obuf.at[k], place(bx, by), lsem.at[3]).start()

        @pl.when(m != k)
        def _(k=k):
            remote(obuf.at[k], place(bx, by), osem_s.at[k], osem_r.at[m], step=2 * k + core).start()

    for copy in outgoing:
        copy.wait_send()
    for ex, e in offsets:
        spread(ex, e, 2)

    @pl.when(w < windows - 1)
    def _():
        onward.wait_send()

    for k in range(half):

        @pl.when(m == k)
        def _(k=k):
            pltpu.make_async_copy(obuf.at[k], place(bx, by), lsem.at[3]).wait()

        @pl.when(m != k)
        def _(k=k):
            done = remote(obuf.at[k], place(k % gx, k // gx), osem_s.at[k], osem_r.at[k], step=partner)
            done.wait_send()
            done.wait_recv()


def blocks(initial_state, source, absorption):
    length = lax.axis_size("step")
    windows = lax.axis_size("win")
    nx, ny, nz = initial_state.shape
    half = length // 2
    gx, reach = half // 2, SWEEPS - 1
    bs, bsy = nx // gx, ny // 2
    ext = min(nx, bs + reach * (1 if gx == 2 else 2))
    ey = bsy + -(-reach // TILE) * TILE
    units = length // 2
    f32 = jnp.float32
    dma = pltpu.SemaphoreType.DMA
    return pl.pallas_call(
        functools.partial(kernel, length, windows, nx, ny, ext, ey),
        out_shape=jax.ShapeDtypeStruct((nx, ny, nz), f32),
        in_specs=[pl.BlockSpec(memory_space=pl.ANY)] * 3,
        out_specs=pl.BlockSpec(memory_space=pl.ANY),
        scratch_shapes=[
            pltpu.VMEM((length, ext, ey, nz), f32),
            pltpu.VMEM((ext, ey, nz), f32),
            pltpu.VMEM((ext, ey, nz), f32),
            pltpu.VMEM((3 * length // 4, ext, ey, nz), f32),
            pltpu.VMEM((units, ext, ey, nz), f32),
            pltpu.VMEM((units, ext, ey, nz), f32),
            pltpu.VMEM((units, ext + 2, ey + 2 * TILE, nz), f32),
            pltpu.VMEM((units, ext + 2, ey + 2 * TILE, nz), f32),
            pltpu.VMEM((ext, ey, nz), f32),
            pltpu.VMEM((bs, TILE, nz), f32),
            pltpu.VMEM((bs, TILE, nz), f32),
            pltpu.VMEM((bs, TILE, nz), f32),
            pltpu.VMEM((bs, TILE, nz), f32),
            pltpu.VMEM((bs, TILE, nz), f32),
            pltpu.VMEM((half, bs, bsy, nz), f32),
            pltpu.VMEM((half, bs, bsy, nz), f32),
            pltpu.VMEM((half, bs, bsy, nz), f32),
            dma((4,)),
            dma((half,)),
            dma((length,)),
            dma((half,)),
            dma((2,)),
            dma((2,)),
            dma((18,)),
            dma((18,)),
            dma((half,)),
            dma((half,)),
            dma((half,)),
            dma((half,)),
        ],
        compiler_params=pltpu.CompilerParams(
            collective_id=0, has_side_effects=True, vmem_limit_bytes=28 * 1024 * 1024
        ),
    )(source[0, 0], initial_state, absorption)[None, None]


def fits(mesh, shape):
    length = mesh.shape["step"]
    if length % 8 or shape[2] != LANES or shape[1] != 4 * TILE:
        return False
    gx = length // 4
    return shape[0] % gx == 0 and shape[0] // gx >= SWEEPS - 1


def solution(mesh):
    def body(initial_state, source, absorption):
        plan = blocks if fits(mesh, initial_state.shape) else per_device
        return plan(initial_state, source, absorption)

    return jax.shard_map(
        body,
        mesh=mesh,
        in_specs=(P(), P("win", "step", None, None, None), P()),
        out_specs=P("win", "step", None, None, None),
        check_vma=False,
    )
```
